512 devices in a mesh: dp: 64 (over y, z), expert: 8 (over x, core).
Axes of the slice: x: 4, y: 8, z: 8, core: 2. Of those that a mesh axis runs over, the one named last changes fastest.
Arguments:
- tokens: bfloat16 [24576, 4096], P('dp'), may hold values from -8 to 8, as said below
- centroids: bfloat16 [512, 4096], P('expert'), may hold values from -8 to 8, as said below
- prices: float32 [512], P('expert'), may hold values from 0 to 259.9922, as said below
- epsilon: float32 [1], replicated, may hold values from 0.125 to 1, as said below
Outputs:
- final_prices: float32 [512], P('expert')
- best_expert: int32 [24576], P('dp')
- holder: int32 [512], P('expert')
- refreshed: bfloat16 [512, 4096], P('expert')
The draws below stay inside these ranges and needn't reach their ends.
Inputs may be any that keep to these rules, and one draw needn't show every extreme that they name: `tokens`: every entry is a whole number. `centroids`: every entry is a whole number. `prices`: distinct multiples of 1/128. `epsilon`: A multiple of 1/8.
All inputs are finite; a program needn't handle non-finite values.
Results may differ from the reference program's by a relative error of at most 0.001.
Values may be sent and summed in bfloat16 or wider, within the bound.
A program may use at most 64 MiB of HBM per device.

```python
import jax
import jax.numpy as jnp
from jax import lax

D = 4096
E = 512
ROUNDS = 3
TOKENS = 24576


def draw_tokens(key, part):
    token_key = jax.random.fold_in(key, 3)
    return jax.random.randint(token_key, (TOKENS, D), -4, 5).astype(jnp.bfloat16)


def draw_centroids(key, part):
    centre_key = jax.random.fold_in(key, 5)
    return jax.random.randint(centre_key, (E, D), -4, 5).astype(jnp.bfloat16)


def draw_prices(key, part):
    ranks = jax.random.permutation(jax.random.fold_in(key, 7), E)
    reserved = (ranks >= E - E // 16).astype(jnp.float32)
    return ranks.astype(jnp.float32) * 0.0078125 + 256.0 * reserved


def draw_epsilon(key, part):
    return jax.random.randint(jax.random.fold_in(key, 11), (1,), 1, 9).astype(jnp.float32) * 0.125


def setup_inputs(seed: int = 0) -> dict:
    splits = jax.random.split(jax.random.key(seed), 5)
    tokens = draw_tokens(jax.random.fold_in(splits[4], 71), 0)
    centroids = draw_centroids(jax.random.fold_in(splits[4], 71), 0)
    prices = draw_prices(jax.random.fold_in(splits[4], 71), 0)
    epsilon = draw_epsilon(jax.random.fold_in(splits[4], 71), 0)
    return {"tokens": tokens, "centroids": centroids, "prices": prices, "epsilon": epsilon}


lowest = -1e30
far_index = 1 << 30


def top_two(values, expert_ids):
    best_value = jnp.max(values, axis=0)
    best_index = jnp.min(jnp.where(values == best_value[None, :], expert_ids[:, None], far_index), axis=0)
    second_value = jnp.max(jnp.where(expert_ids[:, None] == best_index[None, :], lowest, values), axis=0)
    return best_value, best_index, second_value


def reference(tokens, centroids, prices, epsilon):
    scores = lax.dot_general(centroids, tokens, (((1,), (1,)), ((), ())), preferred_element_type=jnp.float32) * 0.015625
    expert_ids = jnp.arange(E, dtype=jnp.int32)
    token_ids = jnp.arange(TOKENS, dtype=jnp.int32)
    current = prices
    for auction_step in range(ROUNDS):
        values = scores - current[:, None]
        best_value, best_index, second_value = top_two(values, expert_ids)
        bids_now = best_value - second_value + epsilon[0]
        claims = expert_ids[:, None] == best_index[None, :]
        top_bid = jnp.max(jnp.where(claims, bids_now[None, :], -1.0), axis=1)
        first_token = jnp.min(jnp.where(claims & (bids_now[None, :] == top_bid[:, None]), token_ids[None, :], far_index), axis=1)
        current = current + jnp.maximum(top_bid, 0.0)
        holder = jnp.where(top_bid > 0, first_token, -1).astype(jnp.int32)
    counts = jnp.sum(claims, axis=1).astype(jnp.float32)
    feature_sums = jnp.dot(claims.astype(jnp.bfloat16), tokens, preferred_element_type=jnp.float32)
    refreshed = (0.5 * centroids.astype(jnp.float32) + 0.5 * feature_sums / jnp.maximum(counts, 1.0)[:, None]).astype(jnp.bfloat16)
    return current, best_index, holder, refreshed
```

```python
import functools

import jax
import jax.numpy as jnp
from jax import lax
from jax.experimental import pallas as pl
from jax.experimental.pallas import tpu as pltpu
from jax.sharding import Mesh
from jax.sharding import PartitionSpec as P

MESH = pl.DeviceIdType.MESH
DP = ("dp_0", "dp_1")
Y, Z, X = "dp_0", "dp_1", "expert"
N = 8
EXPERTS = 512
LOCAL = EXPERTS // N
LOWEST = -1e30
FAR = 1073741824.0
FAR_FIRST = (4, 3, 5, 2, 6, 1, 7)


def modulo(value, n):
    return lax.rem(value, n)


def encode(whole):
    size = jnp.abs(whole)
    level = jnp.floor(size * (1.0 / 128.0))
    coded = (128.0 + (size - 128.0 * level)) * jnp.exp2(level)
    return jnp.where(whole < 0, -coded, coded).astype(jnp.bfloat16)


def decode(coded):
    coded = coded.astype(jnp.float32)
    size = jnp.abs(coded)
    level = jnp.floor(jnp.log2(size) - 7.0)
    whole = 128.0 * level + (size * jnp.exp2(-level) - 128.0)
    return jnp.where(coded < 0, -whole, whole)


def column_of(row):
    return jnp.broadcast_to(row, (128, 128)).T


def row_of(column):
    wide = jnp.broadcast_to(column, (LOCAL, 128))
    return jnp.concatenate([wide, jnp.zeros_like(wide)], axis=0).T[0:1, :]


def kernel(
    tokens_hbm, centroids_hbm, prices_ref, epsilon_ref,
    final_ref, best_ref, holder_ref, out_ref,
    tok, cen, scores, tops, current, best_bid, counts_col,
    vec_out, vec_in, coded, own_sum, sums_in, part, part_in,
    load_sem, send_sem, recv_sem,
):
    me_y, me_z, me_x = (lax.axis_index(a) for a in (Y, Z, X))
    mine = {Y: me_y, Z: me_z, X: me_x}
    partner = me_x + 1 - 2 * modulo(me_x, 2)
    rows = tok.shape[0]
    copies = []

    loads = [pltpu.make_async_copy(centroids_hbm, cen, load_sem.at[0])]
    for j in range(rows // 128):
        at = pl.ds(128 * j, 128)
        loads.append(pltpu.make_async_copy(tokens_hbm.at[at], tok.at[at], load_sem.at[j + 1]))
    for load in loads:
        load.start()

    barrier = pltpu.get_barrier_semaphore()
    for axis in (X, Y, Z):
        for i in range(1, N):
            pl.semaphore_signal(
                barrier, inc=1, device_id={axis: modulo(mine[axis] + i, N)}, device_id_type=MESH
            )

    def send(src, dst, axis, peer):
        k = len(copies)
        copy = pltpu.make_async_remote_copy(
            src_ref=src,
            dst_ref=dst,
            send_sem=send_sem.at[k],
            recv_sem=recv_sem.at[k],
            device_id={axis: peer},
            device_id_type=MESH,
        )
        copy.start()
        copies.append(copy)
        return copy

    own_rows = pl.ds(pl.multiple_of(me_x * LOCAL, LOCAL), LOCAL)
    pair_rows = pl.ds(pl.multiple_of((me_x // 2) * 128, 128), 128)
    current[pair_rows, :] = column_of(prices_ref[:, 0:128])
    loads[0].wait()
    for j in range(rows // 128):
        loads[j + 1].wait()
        block = lax.dot_general(
            cen[...], tok[128 * j : 128 * j + 128, :], (((1,), (1,)), ((), ())),
            preferred_element_type=jnp.float32,
        )
        scores[own_rows, 128 * j : 128 * j + 128] = block * 0.015625

    sub = lax.broadcasted_iota(jnp.int32, (8, rows), 0).astype(jnp.float32)

    def scan_block(first_row, carry):
        best, index, second = carry
        for t in range(8):
            at = pl.ds(pl.multiple_of(first_row + 8 * t, 8), 8)
            price = current[at, :]
            value = scores[at, :] - jnp.concatenate([price] * (rows // 128), axis=1)
            above = value > best
            second = jnp.maximum(second, jnp.minimum(value, best))
            index = jnp.where(above, sub + (first_row + 8 * t).astype(jnp.float32), index)
            best = jnp.maximum(best, value)
        return best, index, second

    def top_two(carry):
        best, index, second = carry
        top = jnp.max(best, axis=0, keepdims=True)
        where = jnp.min(jnp.where(best == top, index, FAR), axis=0, keepdims=True)
        other = jnp.max(jnp.where(index == where, second, best), axis=0, keepdims=True)
        return top, where, other

    low = jnp.full((8, rows), LOWEST, jnp.float32)
    start = (low, jnp.full((8, rows), FAR, jnp.float32), low)
    top, where, other = top_two(scan_block(me_x * LOCAL, start))
    tops[me_x] = jnp.concatenate([top, where, other, prices_ref[...]], axis=0)

    pl.semaphore_wait(barrier, 3 * (N - 1))
    tops_copies = [
        send(tops.at[me_x], tops.at[me_x], X, modulo(me_x + i, N)) for i in FAR_FIRST
    ]
    wide_copies = [
        send(scores.at[own_rows], scores.at[own_rows], X, modulo(me_x + i, N)) for i in (4, 2, 6)
    ]
    pair_copies = [send(scores.at[own_rows], scores.at[own_rows], X, partner)]
    for copy in tops_copies:
        copy.wait_recv()

    lane = lax.broadcasted_iota(jnp.int32, (1, 128), 1)
    price_rows = []
    for e in range(N):
        piece = tops[e]
        top_e, where_e, other_e = piece[0:1], piece[1:2], piece[2:3]
        if e == 0:
            top, where, other = top_e, where_e, other_e
        else:
            above = top_e > top
            other = jnp.where(above, jnp.maximum(other_e, top), jnp.maximum(other, top_e))
            where = jnp.where(above, where_e, where)
            top = jnp.maximum(top, top_e)
        if e % 2:
            price_rows.append(tops[e - 1][3:4, 0:128] + piece[3:4, 0:128])

    def bids_of(top, other):
        return top - other + epsilon_ref[0]

    def exchange_start(k, axis):
        return [
            send(vec_out.at[k], vec_in.at[k, i - 1], axis, modulo(mine[axis] + i, N))
            for i in FAR_FIRST
        ]

    sub_wide = lax.broadcasted_iota(jnp.int32, (8, rows), 0).astype(jnp.float32)

    def price_round(turn, where, bid, price_rows, between):
        where8 = jnp.broadcast_to(where, (8, rows))
        bid8 = jnp.broadcast_to(bid, (8, rows))

        def claim_block(b, carry):
            for t in range(8):
                at = pl.multiple_of(b * 64 + 8 * t, 8)
                hit = jnp.where(sub_wide + at.astype(jnp.float32) == where8, bid8, -1.0)
                most = hit[:, 0:128]
                for c in range(1, rows // 128):
                    most = jnp.maximum(most, hit[:, 128 * c : 128 * c + 128])
                best_bid[pl.ds(at, 8), :] = most
            return carry

        lax.fori_loop(0, EXPERTS // 64, claim_block, 0)
        k = 2 * turn
        for j in range(4):
            cols = slice(128 * j, 128 * j + 128)
            vec_out[k, :, cols] = jnp.max(best_bid[cols, :].T, axis=0, keepdims=True)
        for phase, axis in enumerate((Y, Z)):
            started = exchange_start(k + phase, axis)
            if phase == 1:
                between()
            for copy in started:
                copy.wait_recv()
            found = vec_out[k + phase]
            for i in range(N - 1):
                found = jnp.maximum(found, vec_in[k + phase, i])
            if phase == 0:
                vec_out[k + 1] = found
        price_rows = [
            price_rows[j] + jnp.maximum(found[:, 128 * j : 128 * j + 128], 0.0) for j in range(4)
        ]
        for j in range(4):
            current[128 * j : 128 * j + 128, :] = column_of(price_rows[j])
        return price_rows

    def forward_scores():
        for copy, i in zip(wide_copies, (4, 2, 6)):
            copy.wait_recv()
            source = modulo(me_x - i + N, N)
            at = pl.ds(pl.multiple_of(source * LOCAL, LOCAL), LOCAL)
            pair_copies.append(send(scores.at[at], scores.at[at], X, partner))

    price_rows = price_round(0, where, bids_of(top, other), price_rows, forward_scores)
    for copy in pair_copies:
        copy.wait_recv()

    def full_scan():
        return top_two(
            lax.fori_loop(0, EXPERTS // 64, lambda b, carry: scan_block(b * 64, carry), start)
        )

    top, where, other = full_scan()
    price_rows = price_round(1, where, bids_of(top, other), price_rows, lambda: None)
    top, where, other = full_scan()
    bid = bids_of(top, other)
    best_ref[...] = where.astype(jnp.int32)

    own_ids = (
        lax.broadcasted_iota(jnp.int32, (LOCAL, rows), 0) + me_x * LOCAL
    ).astype(jnp.float32)
    claims = own_ids == jnp.broadcast_to(where, (LOCAL, rows))
    bid_all = jnp.broadcast_to(bid, (LOCAL, rows))
    token_ids = (
        lax.broadcasted_iota(jnp.int32, (LOCAL, rows), 1) + (me_y * N + me_z) * rows
    ).astype(jnp.float32)
    most = jnp.max(jnp.where(claims, bid_all, -1.0), axis=1, keepdims=True)
    first = jnp.min(
        jnp.where(claims & (bid_all == most), token_ids, FAR), axis=1, keepdims=True
    )
    ones = jnp.where(claims, 1.0, 0.0)
    number = jnp.sum(ones, axis=1, keepdims=True)
    most, first, number = row_of(most), row_of(first), row_of(number)

    def put(k):
        vec_out[k] = jnp.concatenate([most, first, number, jnp.zeros_like(most)], axis=1)

    def merge(k, most, first, number):
        for i in range(N - 1):
            piece = vec_in[k, i]
            most_i, first_i, number_i = (piece[:, 128 * c : 128 * c + 128] for c in range(3))
            first = jnp.where(
                most_i > most, first_i, jnp.where(most_i < most, first, jnp.minimum(first, first_i))
            )
            most = jnp.maximum(most, most_i)
            number = number + number_i
        return most, first, number

    put(4)
    last_y = exchange_start(4, Y)

    hot = ones.astype(jnp.bfloat16)
    width = tok.shape[1] // (2 * N)
    bases = (0, N * width)

    def block_at(half, p):
        return pl.ds(pl.multiple_of(bases[half] + p * width, width), width)

    halves = ((Y, Z), (Z, Y))
    reduce_copies = ([], [])
    for i in FAR_FIRST:
        for half, (axis, _) in enumerate(halves):
            p = modulo(mine[axis] + i, N)
            at = block_at(half, p)
            coded[:, at] = encode(jnp.dot(hot, tok[:, at], preferred_element_type=jnp.float32))
            reduce_copies[half].append(
                send(coded.at[:, at], sums_in.at[half, i - 1], axis, p)
            )
    for half, (axis, _) in enumerate(halves):
        own_sum[half] = jnp.dot(
            hot, tok[:, block_at(half, mine[axis])], preferred_element_type=jnp.float32
        )

    for copy in last_y:
        copy.wait_recv()
    most, first, number = merge(4, most, first, number)
    put(5)
    last_z = exchange_start(5, Z)

    def share_at(q):
        return pl.ds(pl.multiple_of((q // 2) * 16, 16), 16), (q - 2 * (q // 2)) * 128

    share_copies = ([], [])
    for half, (_, axis) in enumerate(halves):
        for copy in reduce_copies[half]:
            copy.wait_recv()
        total = own_sum[half]
        for i in range(N - 1):
            total = total + decode(sums_in[half, i])
        part[half] = jnp.floor(total + 0.5)
        for i in FAR_FIRST:
            q = modulo(mine[axis] + i, N)
            share_rows, col = share_at(q)
            share_copies[half].append(
                send(
                    part.at[half, share_rows, pl.ds(pl.multiple_of(col, 128), 128)],
                    part_in.at[half, i - 1], axis, q,
                )
            )

    for copy in last_z:
        copy.wait_recv()
    most, first, number = merge(5, most, first, number)
    own_price = current[own_rows, :]
    own_price = jnp.concatenate([own_price, jnp.zeros_like(own_price)], axis=0).T[0:1, :]
    final = own_price + jnp.maximum(most, 0.0)
    final_ref[...] = final[:, 0:LOCAL]
    holder_ref[...] = jnp.where(most > 0, first, -1.0).astype(jnp.int32)[:, 0:LOCAL]
    counts_col[...] = column_of(jnp.maximum(number, 1.0))[0:LOCAL, :]

    gather_copies = ([], [])
    for half, (base_axis, axis) in enumerate(halves):
        share_rows, col = share_at(mine[axis])
        inner = pl.ds(pl.multiple_of(col, 128), 128)
        outer = pl.ds(pl.multiple_of(bases[half] + mine[base_axis] * width + col, 128), 128)
        for copy in share_copies[half]:
            copy.wait_recv()
        total = part[half, share_rows, inner]
        for i in range(N - 1):
            total = total + part_in[half, i]
        mean = 0.5 * total / counts_col[share_rows, :]
        new = 0.5 * cen[share_rows, outer].astype(jnp.float32) + mean
        out_ref[share_rows, outer] = new.astype(jnp.bfloat16)
        target = out_ref.at[share_rows, outer]
        for i in FAR_FIRST:
            gather_copies[half].append(send(target, target, axis, modulo(mine[axis] + i, N)))

    spread_copies = []
    for half, (axis, _) in enumerate(halves):
        for copy in gather_copies[half]:
            copy.wait_recv()
        target = out_ref.at[:, block_at(half, mine[axis])]
        for i in FAR_FIRST:
            spread_copies.append(send(target, target, axis, modulo(mine[axis] + i, N)))
    for copy in spread_copies:
        copy.wait_recv()
    for copy in copies:
        copy.wait_send()


N_COPIES = 7 + 3 + 4 + 6 * 7 + 4 * 14


def body(tokens, centroids, prices, epsilon):
    rows, depth = tokens.shape
    width = depth // (2 * N)
    odd = lax.axis_index(X) % 2
    line = jnp.where(
        odd == 1,
        jnp.pad(prices, (LOCAL, rows - 2 * LOCAL)),
        jnp.pad(prices, (0, rows - LOCAL)),
    ).reshape(1, rows)
    vmem = pl.BlockSpec(memory_space=pltpu.VMEM)
    final, best, holder, refreshed = pl.pallas_call(
        kernel,
        out_shape=(
            jax.ShapeDtypeStruct((1, LOCAL), jnp.float32),
            jax.ShapeDtypeStruct((1, rows), jnp.int32),
            jax.ShapeDtypeStruct((1, LOCAL), jnp.int32),
            jax.ShapeDtypeStruct((LOCAL, depth), jnp.bfloat16),
        ),
        in_specs=[
            pl.BlockSpec(memory_space=pl.ANY),
            pl.BlockSpec(memory_space=pl.ANY),
            vmem,
            pl.BlockSpec(memory_space=pltpu.SMEM),
        ],
        out_specs=(vmem, vmem, vmem, vmem),
        scratch_shapes=[
            pltpu.VMEM((rows, depth), jnp.bfloat16),
            pltpu.VMEM((LOCAL, depth), jnp.bfloat16),
            pltpu.VMEM((EXPERTS, rows), jnp.float32),
            pltpu.VMEM((N, 4, rows), jnp.float32),
            pltpu.VMEM((EXPERTS, 128), jnp.float32),
            pltpu.VMEM((EXPERTS, 128), jnp.float32),
            pltpu.VMEM((LOCAL, 128), jnp.float32),
            pltpu.VMEM((6, 1, EXPERTS), jnp.float32),
            pltpu.VMEM((6, N - 1, 1, EXPERTS), jnp.float32),
            pltpu.VMEM((LOCAL, depth), jnp.bfloat16),
            pltpu.VMEM((2, LOCAL, width), jnp.float32),
            pltpu.VMEM((2, N - 1, LOCAL, width), jnp.bfloat16),
            pltpu.VMEM((2, LOCAL, width), jnp.float32),
            pltpu.VMEM((2, N - 1, 16, 128), jnp.float32),
            pltpu.SemaphoreType.DMA((1 + rows // 128,)),
            pltpu.SemaphoreType.DMA((N_COPIES,)),
            pltpu.SemaphoreType.DMA((N_COPIES,)),
        ],
        compiler_params=pltpu.CompilerParams(collective_id=0, has_side_effects=True),
    )(tokens, centroids, line, epsilon)
    return final.reshape(-1), best.reshape(-1), holder.reshape(-1), refreshed


def solution(mesh):
    torus = Mesh(mesh.devices.reshape(N, N, mesh.shape["expert"]), (Y, Z, X))
    in_specs = (P(DP, None), P(X, None), P(X), P())
    out_specs = (P(X), P(DP), P(X), P(X, None))
    return jax.shard_map(body, mesh=torus, in_specs=in_specs, out_specs=out_specs, check_vma=False)
```

```python
import functools

import jax
import jax.numpy as jnp
from jax import lax
from jax.experimental import pallas as pl
from jax.experimental.pallas import tpu as pltpu
from jax.sharding import Mesh
from jax.sharding import PartitionSpec as P

MESH = pl.DeviceIdType.MESH
DP = ("dp_0", "dp_1")
Y, Z, X = "dp_0", "dp_1", "expert"
N = 8
EXPERTS = 512
LOCAL = EXPERTS // N
LOWEST = -1e30
FAR = 1073741824.0
FAR_FIRST = (4, 3, 5, 2, 6, 1, 7)


def modulo(value, n):
    return lax.rem(value, n)


def encode(whole):
    size = jnp.abs(whole)
    level = jnp.floor(size * (1.0 / 128.0))
    coded = (128.0 + (size - 128.0 * level)) * jnp.exp2(level)
    return jnp.where(whole < 0, -coded, coded).astype(jnp.bfloat16)


def decode(coded):
    coded = coded.astype(jnp.float32)
    size = jnp.abs(coded)
    level = jnp.floor(jnp.log2(size) - 7.0)
    whole = 128.0 * level + (size * jnp.exp2(-level) - 128.0)
    return jnp.where(coded < 0, -whole, whole)


def column_of(row):
    return jnp.broadcast_to(row, (128, 128)).T


def row_of(column):
    wide = jnp.broadcast_to(column, (LOCAL, 128))
    return jnp.concatenate([wide, jnp.zeros_like(wide)], axis=0).T[0:1, :]


def kernel(
    tokens_hbm, centroids_hbm, prices_hbm, epsilon_ref,
    final_ref, best_ref, holder_ref, out_ref,
    prices_ref, tok, cen, scores, tops, current, best_bid, counts_col,
    vec_out, vec_in, coded, own_sum, sums_in, part, part_in,
    load_sem, send_sem, recv_sem,
):
    me_y, me_z, me_x = (lax.axis_index(a) for a in (Y, Z, X))
    mine = {Y: me_y, Z: me_z, X: me_x}
    partner = me_x + 1 - 2 * modulo(me_x, 2)
    rows = tok.shape[0]
    copies = []

    loads = [pltpu.make_async_copy(centroids_hbm, cen, load_sem.at[0])]
    for j in range(rows // 128):
        at = pl.ds(128 * j, 128)
        loads.append(pltpu.make_async_copy(tokens_hbm.at[at], tok.at[at], load_sem.at[j + 1]))
    loads.append(pltpu.make_async_copy(prices_hbm, prices_ref, load_sem.at[rows // 128 + 1]))
    for load in loads:
        load.start()

    barrier = pltpu.get_barrier_semaphore()
    for axis in (X, Y, Z):
        for i in range(1, N):
            pl.semaphore_signal(
                barrier, inc=1, device_id={axis: modulo(mine[axis] + i, N)}, device_id_type=MESH
            )

    def send(src, dst, axis, peer):
        k = len(copies)
        copy = pltpu.make_async_remote_copy(
            src_ref=src,
            dst_ref=dst,
            send_sem=send_sem.at[k],
            recv_sem=recv_sem.at[k],
            device_id={axis: peer},
            device_id_type=MESH,
        )
        copy.start()
        copies.append(copy)
        return copy

    own_rows = pl.ds(pl.multiple_of(me_x * LOCAL, LOCAL), LOCAL)
    pair_rows = pl.ds(pl.multiple_of((me_x // 2) * 128, 128), 128)
    loads[-1].wait()
    prices = prices_ref[...].reshape(1, LOCAL)
    prices = jnp.concatenate([prices, prices], axis=1)
    upper = lax.broadcasted_iota(jnp.int32, (1, 128), 1) // LOCAL
    prices = jnp.where(upper == modulo(me_x, 2), prices, 0.0)
    current[pair_rows, :] = column_of(prices)
    loads[0].wait()
    for j in range(rows // 128):
        loads[j + 1].wait()
        block = lax.dot_general(
            cen[...], tok[128 * j : 128 * j + 128, :], (((1,), (1,)), ((), ())),
            preferred_element_type=jnp.float32,
        )
        scores[own_rows, 128 * j : 128 * j + 128] = block * 0.015625

    sub = lax.broadcasted_iota(jnp.int32, (8, rows), 0).astype(jnp.float32)

    def scan_block(first_row, carry):
        best, index, second = carry
        for t in range(8):
            at = pl.ds(pl.multiple_of(first_row + 8 * t, 8), 8)
            price = current[at, :]
            value = scores[at, :] - jnp.concatenate([price] * (rows // 128), axis=1)
            above = value > best
            second = jnp.maximum(second, jnp.minimum(value, best))
            index = jnp.where(above, sub + (first_row + 8 * t).astype(jnp.float32), index)
            best = jnp.maximum(best, value)
        return best, index, second

    def top_two(carry):
        best, index, second = carry
        top = jnp.max(best, axis=0, keepdims=True)
        where = jnp.min(jnp.where(best == top, index, FAR), axis=0, keepdims=True)
        other = jnp.max(jnp.where(index == where, second, best), axis=0, keepdims=True)
        return top, where, other

    low = jnp.full((8, rows), LOWEST, jnp.float32)
    start = (low, jnp.full((8, rows), FAR, jnp.float32), low)
    top, where, other = top_two(scan_block(me_x * LOCAL, start))
    tops[me_x] = jnp.concatenate(
        [top, where, other, jnp.concatenate([prices] * (rows // 128), axis=1)], axis=0
    )

    pl.semaphore_wait(barrier, 3 * (N - 1))
    tops_copies = [
        send(tops.at[me_x], tops.at[me_x], X, modulo(me_x + i, N)) for i in FAR_FIRST
    ]
    wide_copies = [
        send(scores.at[own_rows], scores.at[own_rows], X, modulo(me_x + i, N)) for i in (4, 2, 6)
    ]
    pair_copies = [send(scores.at[own_rows], scores.at[own_rows], X, partner)]
    for copy in tops_copies:
        copy.wait_recv()

    lane = lax.broadcasted_iota(jnp.int32, (1, 128), 1)
    price_rows = []
    for e in range(N):
        piece = tops[e]
        top_e, where_e, other_e = piece[0:1], piece[1:2], piece[2:3]
        if e == 0:
            top, where, other = top_e, where_e, other_e
        else:
            above = top_e > top
            other = jnp.where(above, jnp.maximum(other_e, top), jnp.maximum(other, top_e))
            where = jnp.where(above, where_e, where)
            top = jnp.maximum(top, top_e)
        if e % 2:
            price_rows.append(tops[e - 1][3:4, 0:128] + piece[3:4, 0:128])

    def bids_of(top, other):
        return top - other + epsilon_ref[0]

    def exchange_start(k, axis):
        return [
            send(vec_out.at[k], vec_in.at[k, i - 1], axis, modulo(mine[axis] + i, N))
            for i in FAR_FIRST
        ]

    sub_wide = lax.broadcasted_iota(jnp.int32, (8, rows), 0).astype(jnp.float32)

    def price_round(turn, where, bid, price_rows, between):
        where8 = jnp.broadcast_to(where, (8, rows))
        bid8 = jnp.broadcast_to(bid, (8, rows))

        def claim_block(b, carry):
            for t in range(8):
                at = pl.multiple_of(b * 64 + 8 * t, 8)
                hit = jnp.where(sub_wide + at.astype(jnp.float32) == where8, bid8, -1.0)
                most = hit[:, 0:128]
                for c in range(1, rows // 128):
                    most = jnp.maximum(most, hit[:, 128 * c : 128 * c + 128])
                best_bid[pl.ds(at, 8), :] = most
            return carry

        lax.fori_loop(0, EXPERTS // 64, claim_block, 0)
        k = 2 * turn
        for j in range(4):
            cols = slice(128 * j, 128 * j + 128)
            vec_out[k, :, cols] = jnp.max(best_bid[cols, :].T, axis=0, keepdims=True)
        for phase, axis in enumerate((Y, Z)):
            started = exchange_start(k + phase, axis)
            if phase == 1:
                between()
            for copy in started:
                copy.wait_recv()
            found = vec_out[k + phase]
            for i in range(N - 1):
                found = jnp.maximum(found, vec_in[k + phase, i])
            if phase == 0:
                vec_out[k + 1] = found
        price_rows = [
            price_rows[j] + jnp.maximum(found[:, 128 * j : 128 * j + 128], 0.0) for j in range(4)
        ]
        for j in range(4):
            current[128 * j : 128 * j + 128, :] = column_of(price_rows[j])
        return price_rows

    def forward_scores():
        for copy, i in zip(wide_copies, (4, 2, 6)):
            copy.wait_recv()
            source = modulo(me_x - i + N, N)
            at = pl.ds(pl.multiple_of(source * LOCAL, LOCAL), LOCAL)
            pair_copies.append(send(scores.at[at], scores.at[at], X, partner))

    price_rows = price_round(0, where, bids_of(top, other), price_rows, forward_scores)
    for copy in pair_copies:
        copy.wait_recv()

    def full_scan():
        return top_two(
            lax.fori_loop(0, EXPERTS // 64, lambda b, carry: scan_block(b * 64, carry), start)
        )

    top, where, other = full_scan()
    price_rows = price_round(1, where, bids_of(top, other), price_rows, lambda: None)
    top, where, other = full_scan()
    bid = bids_of(top, other)
    best_ref[...] = where.astype(jnp.int32).reshape(rows)

    own_ids = (
        lax.broadcasted_iota(jnp.int32, (LOCAL, rows), 0) + me_x * LOCAL
    ).astype(jnp.float32)
    claims = own_ids == jnp.broadcast_to(where, (LOCAL, rows))
    bid_all = jnp.broadcast_to(bid, (LOCAL, rows))
    token_ids = (
        lax.broadcasted_iota(jnp.int32, (LOCAL, rows), 1) + (me_y * N + me_z) * rows
    ).astype(jnp.float32)
    most = jnp.max(jnp.where(claims, bid_all, -1.0), axis=1, keepdims=True)
    first = jnp.min(
        jnp.where(claims & (bid_all == most), token_ids, FAR), axis=1, keepdims=True
    )
    ones = jnp.where(claims, 1.0, 0.0)
    number = jnp.sum(ones, axis=1, keepdims=True)
    most, first, number = row_of(most), row_of(first), row_of(number)

    def put(k):
        vec_out[k] = jnp.concatenate([most, first, number, jnp.zeros_like(most)], axis=1)

    def merge(k, most, first, number):
        for i in range(N - 1):
            piece = vec_in[k, i]
            most_i, first_i, number_i = (piece[:, 128 * c : 128 * c + 128] for c in range(3))
            first = jnp.where(
                most_i > most, first_i, jnp.where(most_i < most, first, jnp.minimum(first, first_i))
            )
            most = jnp.maximum(most, most_i)
            number = number + number_i
        return most, first, number

    put(4)
    last_y = exchange_start(4, Y)

    hot = ones.astype(jnp.bfloat16)
    width = tok.shape[1] // (2 * N)
    bases = (0, N * width)

    def block_at(half, p):
        return pl.ds(pl.multiple_of(bases[half] + p * width, width), width)

    halves = ((Y, Z), (Z, Y))
    reduce_copies = ([], [])
    for i in FAR_FIRST:
        for half, (axis, _) in enumerate(halves):
            p = modulo(mine[axis] + i, N)
            at = block_at(half, p)
            coded[:, at] = encode(jnp.dot(hot, tok[:, at], preferred_element_type=jnp.float32))
            reduce_copies[half].append(
                send(coded.at[:, at], sums_in.at[half, i - 1], axis, p)
            )
    for half, (axis, _) in enumerate(halves):
        own_sum[half] = jnp.dot(
            hot, tok[:, block_at(half, mine[axis])], preferred_element_type=jnp.float32
        )

    for copy in last_y:
        copy.wait_recv()
    most, first, number = merge(4, most, first, number)
    put(5)
    last_z = exchange_start(5, Z)

    def share_at(q):
        return pl.ds(pl.multiple_of((q // 2) * 16, 16), 16), (q - 2 * (q // 2)) * 128

    share_copies = ([], [])
    for half, (_, axis) in enumerate(halves):
        for copy in reduce_copies[half]:
            copy.wait_recv()
        total = own_sum[half]
        for i in range(N - 1):
            total = total + decode(sums_in[half, i])
        part[half] = jnp.floor(total + 0.5)
        for i in FAR_FIRST:
            q = modulo(mine[axis] + i, N)
            share_rows, col = share_at(q)
            share_copies[half].append(
                send(
                    part.at[half, share_rows, pl.ds(pl.multiple_of(col, 128), 128)],
                    part_in.at[half, i - 1], axis, q,
                )
            )

    for copy in last_z:
        copy.wait_recv()
    most, first, number = merge(5, most, first, number)
    own_price = current[own_rows, :]
    own_price = jnp.concatenate([own_price, jnp.zeros_like(own_price)], axis=0).T[0:1, :]
    final = own_price + jnp.maximum(most, 0.0)
    final_ref[...] = final[:, 0:LOCAL].reshape(LOCAL)
    holder_ref[...] = jnp.where(most > 0, first, -1.0).astype(jnp.int32)[:, 0:LOCAL].reshape(LOCAL)
    counts_col[...] = column_of(jnp.maximum(number, 1.0))[0:LOCAL, :]

    gather_copies = ([], [])
    for half, (base_axis, axis) in enumerate(halves):
        share_rows, col = share_at(mine[axis])
        inner = pl.ds(pl.multiple_of(col, 128), 128)
        outer = pl.ds(pl.multiple_of(bases[half] + mine[base_axis] * width + col, 128), 128)
        for copy in share_copies[half]:
            copy.wait_recv()
        total = part[half, share_rows, inner]
        for i in range(N - 1):
            total = total + part_in[half, i]
        mean = 0.5 * total / counts_col[share_rows, :]
        new = 0.5 * cen[share_rows, outer].astype(jnp.float32) + mean
        out_ref[share_rows, outer] = new.astype(jnp.bfloat16)
        target = out_ref.at[share_rows, outer]
        for i in FAR_FIRST:
            gather_copies[half].append(send(target, target, axis, modulo(mine[axis] + i, N)))

    spread_copies = []
    for half, (axis, _) in enumerate(halves):
        for copy in gather_copies[half]:
            copy.wait_recv()
        target = out_ref.at[:, block_at(half, mine[axis])]
        for i in FAR_FIRST:
            spread_copies.append(send(target, target, axis, modulo(mine[axis] + i, N)))
    for copy in spread_copies:
        copy.wait_recv()
    for copy in copies:
        copy.wait_send()


N_COPIES = 7 + 3 + 4 + 6 * 7 + 4 * 14


def hand_over(*refs):
    count = (len(refs) - 1) // 2
    moves = [
        pltpu.make_async_copy(refs[k], refs[count + k], refs[-1].at[k]) for k in range(count)
    ]
    for move in moves:
        move.start()
    for move in moves:
        move.wait()


def body(tokens, centroids, prices, epsilon):
    rows, depth = tokens.shape
    width = depth // (2 * N)
    vmem = pl.BlockSpec(memory_space=pltpu.VMEM)
    outside = pl.BlockSpec(memory_space=pltpu.HBM)
    results = (
        jax.ShapeDtypeStruct((LOCAL,), jnp.float32),
        jax.ShapeDtypeStruct((rows,), jnp.int32),
        jax.ShapeDtypeStruct((LOCAL,), jnp.int32),
        jax.ShapeDtypeStruct((LOCAL, depth), jnp.bfloat16),
    )
    found = pl.pallas_call(
        kernel,
        out_shape=results,
        in_specs=[outside] * 3 + [pl.BlockSpec(memory_space=pltpu.SMEM)],
        out_specs=(vmem,) * 4,
        scratch_shapes=[
            pltpu.VMEM((LOCAL,), jnp.float32),
            pltpu.VMEM((rows, depth), jnp.bfloat16),
            pltpu.VMEM((LOCAL, depth), jnp.bfloat16),
            pltpu.VMEM((EXPERTS, rows), jnp.float32),
            pltpu.VMEM((N, 4, rows), jnp.float32),
            pltpu.VMEM((EXPERTS, 128), jnp.float32),
            pltpu.VMEM((EXPERTS, 128), jnp.float32),
            pltpu.VMEM((LOCAL, 128), jnp.float32),
            pltpu.VMEM((6, 1, EXPERTS), jnp.float32),
            pltpu.VMEM((6, N - 1, 1, EXPERTS), jnp.float32),
            pltpu.VMEM((LOCAL, depth), jnp.bfloat16),
            pltpu.VMEM((2, LOCAL, width), jnp.float32),
            pltpu.VMEM((2, N - 1, LOCAL, width), jnp.bfloat16),
            pltpu.VMEM((2, LOCAL, width), jnp.float32),
            pltpu.VMEM((2, N - 1, 16, 128), jnp.float32),
            pltpu.SemaphoreType.DMA((2 + rows // 128,)),
            pltpu.SemaphoreType.DMA((N_COPIES,)),
            pltpu.SemaphoreType.DMA((N_COPIES,)),
        ],
        compiler_params=pltpu.CompilerParams(collective_id=0, has_side_effects=True, vmem_limit_bytes=24 * 2**20),
    )(*(pltpu.with_memory_space_constraint(a, pltpu.HBM) for a in (tokens, centroids, prices)), epsilon)
    return pl.pallas_call(
        hand_over,
        out_shape=results,
        in_specs=[vmem] * 4,
        out_specs=(outside,) * 4,
        scratch_shapes=[pltpu.SemaphoreType.DMA((4,))],
        compiler_params=pltpu.CompilerParams(vmem_limit_bytes=8 * 2**20),
    )(*found)


def solution(mesh):
    torus = Mesh(mesh.devices.reshape(N, N, mesh.shape["expert"]), (Y, Z, X))
    in_specs = (P(DP, None), P(X, None), P(X), P())
    out_specs = (P(X), P(DP), P(X), P(X, None))
    return jax.shard_map(body, mesh=torus, in_specs=in_specs, out_specs=out_specs, check_vma=False)
```
